32 devices in a mesh: pair: 8 (over y, x, core), tm: 4 (over z).
Axes of the slice: x: 2, y: 2, z: 4, core: 2. Of those that a mesh axis runs over, the one named last changes fastest.
Arguments:
- three_centre: bfloat16 [1536, 16384], P(None, 'pair'), may hold values from -0.09375 to 0.09375
- root_coulomb: bfloat16 [1536, 1536], P(('pair', 'tm')), may hold values from -0.15625 to 0.15625
- occ_depth: float32 [256], replicated, may hold values from 0.1 to 1
- vir_energy: float32 [1024], replicated, may hold values from 0.01 to 500
- occ_block: int32 [64], P('pair'), may hold values from 0 to 15
- vir_block: int32 [64], P('pair'), may hold values from 0 to 63
Outputs:
- screened: float32 [4, 1536, 1536], P('tm', 'pair')
The draws below stay inside these ranges and needn't reach their ends.
All inputs are finite; a program needn't handle non-finite values.
Results may differ from the reference program's by a relative error of at most 0.003.
Values may be sent and summed in bfloat16 or wider, within the bound.
No kernel may reach another device: no remote copies, remote signals or barrier semaphores. Data moves between devices by JAX's collectives and lax.ppermute only.
A program may use at most 128 MiB of HBM per device.

```python
import math
import jax
import jax.numpy as jnp
from jax import lax

NAUX = 1536
OB = 16
VB = 16
NOB = 16
NVB = 64
NBLK = 64
PAIRS = 16384
TIMES = 4


def with_ends(result, own_key, least, largest):
    spot = [jax.random.randint(jax.random.fold_in(own_key, axis), (), 0, length) for axis, length in enumerate(result.shape)]
    longest = result.shape.index(max(result.shape))
    neighbour = spot[:longest] + [(spot[longest] + 1) % result.shape[longest]] + spot[longest + 1:]
    return result.at[tuple(spot)].set(least).at[tuple(neighbour)].set(largest)


def levels(key, extent, split, smallest, high):
    loudness = 1.0
    for axis_at, blocks in split:
        steps = jax.random.uniform(jax.random.fold_in(jax.random.fold_in(key, 6), axis_at), (blocks,), jnp.float32, smallest / len(split), high / len(split))
        loudness = loudness * jnp.repeat(jnp.exp(steps), extent[axis_at] // blocks).reshape((-1,) + (1,) * (len(extent) - 1 - axis_at))
    return loudness


def scatter_about(stream_key, extent, spread, limit, shards=(), kind=jnp.bfloat16):
    level = levels(stream_key, extent, shards, -0.22, 0.18) if shards else 1.0
    result = jax.random.normal(stream_key, extent, jnp.float32) * spread * level
    return jnp.minimum(jnp.maximum(result, -limit), limit).astype(kind)


def setup_inputs(seed: int = 0) -> dict:
    splits = jax.random.split(jax.random.key(seed), 7)
    return {
        "three_centre": scatter_about(splits[0], (NAUX, PAIRS), (PAIRS // 4) ** -0.5, 0.09375, ((1, 8),)),
        "root_coulomb": scatter_about(splits[1], (NAUX, NAUX), NAUX ** -0.5, 0.15625, ((0, 32),)),
        "occ_depth": jnp.clip(jnp.exp(jax.random.uniform(splits[2], (NOB * OB,), jnp.float32, math.log(0.1), math.log(1.0))), 0.1, 1.0),
        "vir_energy": jnp.clip(jnp.exp(jax.random.uniform(splits[3], (NVB * VB,), jnp.float32, math.log(0.01), math.log(500.0))), 0.01, 500.0),
        "occ_block": with_ends(jax.random.randint(splits[4], (NBLK,), 0, NOB), jax.random.fold_in(splits[4], 1), 0, NOB - 1).astype(jnp.int32),
        "vir_block": with_ends(jax.random.randint(splits[5], (NBLK,), 0, NVB), jax.random.fold_in(splits[5], 1), 0, NVB - 1).astype(jnp.int32),
    }


log_span = math.log(5000.0)


def reference(three_centre, root_coulomb, occ_depth, vir_energy, occ_block, vir_block):
    occ_sel = occ_depth.reshape(NOB, OB)[occ_block.astype(jnp.int32)]
    vir_sel = vir_energy.reshape(NVB, VB)[vir_block.astype(jnp.int32)]
    gap = (occ_sel[:, :, None] + vir_sel[:, None, :]).reshape(-1)
    whole = three_centre.astype(jnp.float32)
    steps_t = jnp.arange(TIMES).astype(jnp.float32)
    taus = 0.002 * jnp.exp(steps_t * (log_span / max(TIMES - 1, 1)))
    omegas = (steps_t + 0.5) / TIMES
    coef = 2.4 * omegas[:, None] * jnp.cos(jnp.pi * omegas[:, None] * (steps_t[None, :] + 0.5))
    decays = jnp.exp(-gap[None, :] * taus[:, None])
    freq_weight = jnp.dot(coef, decays, precision=lax.Precision.HIGHEST)
    root_whole = root_coulomb.astype(jnp.float32)
    outputs = []
    for index in range(TIMES):
        weighted = (whole * freq_weight[index][None, :]).astype(jnp.bfloat16).astype(jnp.float32)
        chi = jnp.dot(weighted, whole.T, precision=lax.Precision.HIGHEST)
        chi_low = chi.astype(jnp.bfloat16).astype(jnp.float32)
        outputs.append(jnp.dot(chi_low, root_whole, precision=lax.Precision.HIGHEST))
    return jnp.stack(outputs)
```

```python
import functools
import math

import numpy as np

import jax
import jax.numpy as jnp
from jax import lax
from jax.experimental import pallas as pl
from jax.experimental.pallas import tpu as pltpu
from jax.sharding import PartitionSpec as P


OB = 16
VB = 16
LANES = 128
SUBLANES = 16
TILE = 512
SPLIT = 512


AXES = ("pair", "tm")
LOG_SPAN = math.log(5000.0)


def popcount(mask):
    return bin(mask).count("1")


def time_tables(n_times):
    steps = np.arange(n_times).astype(np.float32)
    taus = (0.002 * np.exp(steps * np.float32(LOG_SPAN / max(n_times - 1, 1)))).astype(np.float32)
    omegas = ((steps + 0.5) / n_times).astype(np.float32)
    angle = np.float32(np.pi) * omegas[:, None] * (steps[None, :] + np.float32(0.5))
    coef = (np.float32(2.4) * omegas[:, None] * np.cos(angle)).astype(np.float32)
    return [float(t) for t in taus], [[float(c) for c in row] for row in coef]


def weights_kernel(taus, coef, occ_block, vir_block, occ_ref, vir_ref, w_ref):
    n_blocks = w_ref.shape[0]
    shape = (n_blocks, LANES)
    row = lax.broadcasted_iota(jnp.int32, shape, 0)
    lane = lax.broadcasted_iota(jnp.int32, shape, 1)

    def table_rows(block_ref, table_ref, width):
        chosen = jnp.zeros(shape, jnp.int32)
        for k in range(n_blocks):
            chosen = jnp.where(row == k, block_ref[k], chosen)
        per_group = LANES // width
        found = jnp.zeros(shape, jnp.float32)
        for group in range(table_ref.shape[1] // LANES):
            part = table_ref[:, group * LANES : (group + 1) * LANES]
            found += jnp.where(lane // width + group * per_group == chosen, part, 0.0)
        shift = width
        while shift < LANES:
            found += pltpu.roll(found, shift, 1)
            shift *= 2
        return found

    occ = table_rows(occ_block, occ_ref, OB)
    vir = table_rows(vir_block, vir_ref, VB)
    mine = lax.axis_index("tm")
    n_times = len(taus)
    for part in range(OB * VB // LANES):
        level = jnp.take_along_axis(occ, lane // VB + part * (LANES // VB), axis=1)
        gap = level + vir
        total = jnp.zeros(shape, jnp.float32)
        for i in range(n_times):
            factor = jnp.float32(0.0)
            for j in range(n_times):
                factor = jnp.where(mine == j, jnp.float32(coef[j][i]), factor)
            total += factor * jnp.exp(-gap * taus[i])
        w_ref[:, part * LANES : (part + 1) * LANES] = total


def scale_rows(scaled, new, source, w_ref):
    width = w_ref.shape[1]
    for k in range(w_ref.shape[0]):
        cols = pl.ds(k * width, width)
        scaled[new, cols] = (source(cols).astype(jnp.float32) * w_ref[k : k + 1, :]).astype(jnp.bfloat16)


def multiply(scaled, right, here, outs, arrived=None):
    total = lax.dot_general(scaled[...], right, (((1,), (1,)), ((), ())), preferred_element_type=jnp.float32)
    rows = outs[0].shape[0]
    for b, out in enumerate(outs):
        value = total[b * rows : (b + 1) * rows]
        if arrived:
            value += arrived[b][:, here].astype(jnp.float32)
        out[:, here] = value.astype(out.dtype)


def blocks_of(layers, n_pair, naux, z):
    if layers == 1:
        return [(0, 0, naux)]
    height = naux // (layers * n_pair)
    return [
        ((p * layers + jnp.bitwise_xor(z, layer)) * height, (layer * n_pair + p) * height, height)
        for layer in range(layers)
        for p in range(n_pair)
    ]


def first_kernel(taus, coef, layers, masks, occ_block, vir_block, occ, vir, source, *refs):
    count = len(masks)
    w_ref, held, outs = refs[0], refs[1], refs[2 : 2 + count]
    occ_b, vir_b, occ_t, vir_t, left, scaled, sems = refs[2 + count :]
    naux, rows = held.shape[0], outs[0].shape[0]
    me, z, n_pair = lax.axis_index("pair"), lax.axis_index("tm"), lax.axis_size("pair")
    small = ((occ_block, occ_b), (vir_block, vir_b), (occ, occ_t), (vir, vir_t))
    pairs = list(small)
    for b, mask in enumerate(masks):
        first = pl.multiple_of(jnp.bitwise_xor(me, mask) * rows, SUBLANES)
        pairs.append((source.at[pl.ds(first, rows), :], left.at[pl.ds(b * rows, rows), :]))
    blocks = blocks_of(layers, n_pair, naux, z)
    for old, new, length in blocks:
        pairs.append((source.at[pl.ds(pl.multiple_of(old, SUBLANES), length), :], held.at[pl.ds(new, length), :]))
    copies = [pltpu.make_async_copy(here, there, sems.at[i]) for i, (here, there) in enumerate(pairs)]
    for copy in copies:
        copy.start()
    for copy in copies[: len(small)]:
        copy.wait()
    weights_kernel(taus, coef, occ_b, vir_b, occ_t, vir_t, w_ref)
    for b in range(count):
        copies[len(small) + b].wait()
        here = pl.ds(b * rows, rows)
        scale_rows(scaled, here, lambda cols: left[here, cols], w_ref)
    waiting = list(zip(copies[len(small) + count :], blocks))
    tile = math.gcd(naux, TILE)
    for n in range(naux // tile):
        while waiting and waiting[0][1][1] < (n + 1) * tile:
            waiting.pop(0)[0].wait()
        here = pl.ds(n * tile, tile)
        multiply(scaled, held[here, :], here, outs)


def first_rows(three_centre, occ_depth, vir_energy, occ_block, vir_block, masks, rows, layers, n_times):
    taus, coef = time_tables(n_times)
    naux, depth = three_centre.shape
    count = len(masks)
    vmem = pl.BlockSpec(memory_space=pltpu.VMEM)
    operands = (occ_block, vir_block, occ_depth.reshape(1, -1), vir_energy.reshape(1, -1), three_centre)
    n_copies = 4 + count + (1 if layers == 1 else layers * lax.axis_size("pair"))
    results = pl.pallas_call(
        functools.partial(first_kernel, taus, coef, layers, masks),
        out_shape=[
            pltpu.VMEM((occ_block.shape[0], OB * VB), jnp.float32),
            pltpu.VMEM(three_centre.shape, three_centre.dtype),
        ]
        + [jax.ShapeDtypeStruct((rows, naux), jnp.bfloat16)] * count,
        in_specs=[pl.BlockSpec(memory_space=pltpu.HBM)] * len(operands),
        out_specs=[vmem] * (2 + count),
        scratch_shapes=[pltpu.SMEM(occ_block.shape, jnp.int32), pltpu.SMEM(vir_block.shape, jnp.int32)]
        + [pltpu.VMEM(v.shape, jnp.float32) for v in operands[2:4]]
        + [pltpu.VMEM((count * rows, depth), jnp.bfloat16)] * 2
        + [pltpu.SemaphoreType.DMA((n_copies,))],
        name="first",
        compiler_params=pltpu.CompilerParams(vmem_limit_bytes=24 * 2**20),
        cost_estimate=pl.CostEstimate(
            flops=2 * count * rows * naux * depth, bytes_accessed=2 * three_centre.size, transcendentals=10**4
        ),
    )(*[pltpu.with_memory_space_constraint(v, pltpu.HBM) for v in operands])
    return results[0], results[1], results[2:]


def partial_kernel(masks, received, layers, w_ref, held, *refs):
    count = len(masks)
    arrived = refs[: count if received else 0]
    outs, scaled = refs[-1 - count : -1], refs[-1]
    rows, naux = outs[0].shape
    me, z, n_pair = lax.axis_index("pair"), lax.axis_index("tm"), lax.axis_size("pair")
    height = rows // layers
    for b, mask in enumerate(masks):
        owner = jnp.bitwise_xor(me, mask)
        for part in range(layers):
            row = owner if layers == 1 else jnp.bitwise_xor(z, part) * n_pair + owner
            old = pl.ds(pl.multiple_of(row * height, SUBLANES), height)
            scale_rows(scaled, pl.ds(b * rows + part * height, height), lambda cols: held[old, cols], w_ref)
    tile = math.gcd(naux, TILE)
    for n in range(naux // tile):
        here = pl.ds(n * tile, tile)
        multiply(scaled, held[here, :], here, outs, arrived)


def partial_rows(held, weights, masks, dtypes, rows, layers, arrived=None):
    naux, depth = held.shape
    count = len(masks)
    vmem = pl.BlockSpec(memory_space=pltpu.VMEM)
    operands = [weights, held] + (arrived or [])
    return pl.pallas_call(
        functools.partial(partial_kernel, masks, arrived is not None, layers),
        in_specs=[vmem] * len(operands),
        out_specs=[vmem] * count,
        scratch_shapes=[pltpu.VMEM((count * rows, depth), jnp.bfloat16)],
        out_shape=[jax.ShapeDtypeStruct((rows, naux), t) for t in dtypes],
        name="partial",
        compiler_params=pltpu.CompilerParams(vmem_limit_bytes=16 * 2**20),
        cost_estimate=pl.CostEstimate(
            flops=2 * count * rows * naux * depth,
            bytes_accessed=2 * (naux + count * rows) * depth + 4 * count * rows * naux,
            transcendentals=0,
        ),
    )(*[pltpu.with_memory_space_constraint(v, pltpu.VMEM) for v in operands[:2]], *operands[2:])


def lay(root, first_layer, last_layer, plan, pieces, height):
    me, z, n_pair = lax.axis_index("pair"), lax.axis_index("tm"), lax.axis_size("pair")
    for piece, (column, needed, blocks) in zip(pieces, plan):
        cols = pl.ds(column, piece.shape[1])

        def move():
            for i, (mask, layer) in enumerate(blocks):
                if first_layer <= layer < last_layer:
                    target = (jnp.bitwise_xor(me, mask) + (layer - first_layer) * n_pair) * height
                    root[pl.ds(pl.multiple_of(target, SUBLANES), height), cols] = piece[i * height : (i + 1) * height, :]

        if needed is None:
            move()
        else:
            pl.when(needed(z))(move)


def choose(pieces, first_layer, last_layer):
    kept = [p for p in pieces if any(first_layer <= layer < last_layer for _, layer in p[2])]
    return [p[:3] for p in kept], [p[3] for p in kept]


def collect_kernel(plan, last_layer, height, *refs):
    lay(refs[-1], 0, last_layer, plan, refs[:-1], height)


def collect(pieces, last_layer, height, naux):
    plan, values = choose(pieces, 0, last_layer)
    rows = last_layer * lax.axis_size("pair") * height
    vmem = pl.BlockSpec(memory_space=pltpu.VMEM)
    return pl.pallas_call(
        functools.partial(collect_kernel, plan, last_layer, height),
        in_specs=[vmem] * len(values),
        out_specs=vmem,
        out_shape=pltpu.VMEM((rows, naux), values[0].dtype),
        name="collect",
        compiler_params=pltpu.CompilerParams(vmem_limit_bytes=8 * 2**20),
        cost_estimate=pl.CostEstimate(flops=10**9, bytes_accessed=4 * rows * naux, transcendentals=0),
    )(*values)


def screen_kernel(n_terms, *refs):
    terms = refs[:n_terms]
    root, out, chi = refs[n_terms:]
    value = terms[0][...].astype(jnp.float32)
    for term in terms[1:]:
        value += term[...].astype(jnp.float32)
    chi[...] = value.astype(jnp.bfloat16)
    tile = math.gcd(out.shape[1], TILE)
    for n in range(out.shape[1] // tile):
        cols = pl.ds(n * tile, tile)
        out[:, cols] = jnp.dot(chi[:, : root.shape[0]], root[:, cols], preferred_element_type=jnp.float32)


def screen(terms, root):
    rows, naux = terms[0].shape
    vmem = pl.BlockSpec(memory_space=pltpu.VMEM)
    return pl.pallas_call(
        functools.partial(screen_kernel, len(terms)),
        in_specs=[vmem] * (len(terms) + 1),
        out_specs=[vmem] * 2,
        out_shape=[
            jax.ShapeDtypeStruct((rows, root.shape[1]), jnp.float32),
            jax.ShapeDtypeStruct((rows, naux), jnp.bfloat16),
        ],
        name="screen",
        compiler_params=pltpu.CompilerParams(vmem_limit_bytes=8 * 2**20),
        cost_estimate=pl.CostEstimate(
            flops=2 * rows * root.size, bytes_accessed=2 * root.size + 6 * rows * naux, transcendentals=0
        ),
    )(*terms, root)


def finish_kernel(plan, layer, height, total, chi, *refs):
    pieces, (out, root, staged, sems) = refs[: len(plan)], refs[len(plan) :]
    lay(root, layer, layer + 1, plan, pieces, height)
    depth = root.shape[0]
    tile = math.gcd(out.shape[2], TILE)
    copies = []
    for n in range(out.shape[2] // tile):
        cols = pl.ds(n * tile, tile)
        staged[:, cols] = total[:, cols] + jnp.dot(
            chi[:, chi.shape[1] - depth :], root[:, cols], preferred_element_type=jnp.float32
        )
        copies.append(pltpu.make_async_copy(staged.at[:, cols], out.at[0, :, cols], sems.at[n]))
        copies[-1].start()
    for copy in copies:
        copy.wait()


def finish(total, chi, pieces, layer, height):
    rows, naux = total.shape
    plan, values = choose(pieces, layer, layer + 1)
    depth = lax.axis_size("pair") * height
    vmem = pl.BlockSpec(memory_space=pltpu.VMEM)
    return pl.pallas_call(
        functools.partial(finish_kernel, plan, layer, height),
        in_specs=[vmem] * (2 + len(values)),
        out_specs=pl.BlockSpec(memory_space=pltpu.HBM),
        out_shape=jax.ShapeDtypeStruct((1, rows, naux), jnp.float32),
        scratch_shapes=[
            pltpu.VMEM((depth, naux), jnp.bfloat16),
            pltpu.VMEM((rows, naux), jnp.float32),
            pltpu.SemaphoreType.DMA((naux // math.gcd(naux, TILE),)),
        ],
        name="finish",
        compiler_params=pltpu.CompilerParams(vmem_limit_bytes=8 * 2**20),
        cost_estimate=pl.CostEstimate(
            flops=2 * rows * depth * naux, bytes_accessed=2 * depth * naux + 8 * rows * naux, transcendentals=0
        ),
    )(total, chi, *values)


def swap(value, mask):
    n_pair = lax.axis_size("pair")
    return lax.ppermute(value, "pair", [(p, p ^ mask) for p in range(n_pair)])


def along(value, moves):
    return lax.ppermute(value, "tm", moves)


def is_inner(z):
    return jnp.logical_or(z == 1, z == 2)


def is_outer(z):
    return jnp.logical_or(z == 0, z == 3)


def gather_root(root_coulomb):
    n_pair, n_tm = lax.axis_size("pair"), lax.axis_size("tm")
    masks = [2 * m for m in range(n_pair // 2)]
    near = [root_coulomb] + [swap(root_coulomb, m) for m in masks[1:]]
    plane = jnp.concatenate([rows[:, SPLIT:] for rows in near], axis=0)
    middle, outward = [(1, 2), (2, 1)], [(1, 0), (2, 3)]
    first = along(plane, [(z, z ^ 1) for z in range(n_tm)])
    second = along(plane, middle)
    inner = along(first, middle)
    outer = along(second, outward)
    last = along(inner, outward)
    pieces = []

    def both(column, needed, blocks, value):
        pieces.append((column, needed, blocks, value))
        pieces.append((column, needed, [(m ^ 1, layer) for m, layer in blocks], swap(value, 1)))

    for value, layer, needed in (
        (plane, 0, None),
        (first, 1, None),
        (second, 3, is_inner),
        (inner, 2, is_inner),
        (outer, 2, is_outer),
        (last, 3, is_outer),
    ):
        both(SPLIT, needed, [(m, layer) for m in masks], value)
    if SPLIT:
        tall = root_coulomb[:, :SPLIT]
        layers = range(n_tm)
        far = [tall] + [along(tall, [(z, z ^ m) for z in layers]) for m in layers[1:]]
        tower = jnp.concatenate(far, axis=0)
        for mask in masks:
            value = swap(tower, mask) if mask else tower
            both(0, None, [(mask, layer) for layer in layers], value)
    return pieces


def shards(layers, three_centre, root_coulomb, occ_depth, vir_energy, occ_block, vir_block):
    n_pair, n_tm = lax.axis_size("pair"), lax.axis_size("tm")
    height = root_coulomb.shape[0]
    rows = three_centre.shape[0] // n_pair
    if layers == 1:
        root = lax.all_gather(root_coulomb, AXES, axis=0, tiled=True)
    else:
        pieces = gather_root(root_coulomb)
        root = collect(pieces, layers - 1, height, three_centre.shape[0])
    halves = []
    groups = chip_groups(n_pair, rows)
    for g, group in enumerate(groups):
        masks = [2 * m + 1 for m in group]
        if g == 0:
            weights, held, parts = first_rows(
                three_centre, occ_depth, vir_energy, occ_block, vir_block, masks, rows, layers, n_tm
            )
        else:
            parts = partial_rows(held, weights, masks, [jnp.bfloat16] * len(group), rows, layers)
        halves.append([swap(part, 1) for part in parts])
    terms = []
    for g, group in enumerate(groups):
        dtypes = [jnp.bfloat16 if m else jnp.float32 for m in group]
        sums = partial_rows(held, weights, [2 * m for m in group], dtypes, rows, layers, halves[g])
        terms += [swap(part, 2 * m) if m else part for m, part in zip(group, sums)]
    total, chi = screen(terms, root)
    if layers == 1:
        return total[None]
    return finish(total, chi, pieces, layers - 1, height)


def chip_groups(n_pair, rows):
    chips = sorted(range(n_pair // 2), key=lambda m: -popcount(m))
    size = max(1, min(len(chips), 384 // rows))
    return [chips[i : i + size] for i in range(0, len(chips), size)]


def solution(mesh):
    n_pair, n_tm = mesh.shape["pair"], mesh.shape["tm"]
    in_specs = (P(None, "pair"), P(("pair", "tm"), None), P(), P(), P("pair"), P("pair"))
    out_specs = P("tm", "pair", None)

    def step(*args):
        height = args[1].shape[0] // (n_pair * n_tm)
        line = n_tm == 4 and n_pair == 8 and height % SUBLANES == 0
        body = functools.partial(shards, n_tm if line else 1)
        return jax.shard_map(body, mesh=mesh, in_specs=in_specs, out_specs=out_specs, check_vma=False)(*args)

    return step
```

```python
import functools
import math

import numpy as np

import jax
import jax.numpy as jnp
from jax import lax
from jax.experimental import pallas as pl
from jax.experimental.pallas import tpu as pltpu
from jax.sharding import PartitionSpec as P


OB = 16
VB = 16
LANES = 128
SUBLANES = 16
TILE = 512
SPLIT = 768


AXES = ("pair", "tm")
LOG_SPAN = math.log(5000.0)


def popcount(mask):
    return bin(mask).count("1")


def time_tables(n_times):
    steps = np.arange(n_times).astype(np.float32)
    taus = (0.002 * np.exp(steps * np.float32(LOG_SPAN / max(n_times - 1, 1)))).astype(np.float32)
    omegas = ((steps + 0.5) / n_times).astype(np.float32)
    angle = np.float32(np.pi) * omegas[:, None] * (steps[None, :] + np.float32(0.5))
    coef = (np.float32(2.4) * omegas[:, None] * np.cos(angle)).astype(np.float32)
    return [float(t) for t in taus], [[float(c) for c in row] for row in coef]


def weights_kernel(taus, coef, occ_block, vir_block, occ_ref, vir_ref, w_ref):
    n_blocks = w_ref.shape[0]
    shape = (n_blocks, LANES)
    row = lax.broadcasted_iota(jnp.int32, shape, 0)
    lane = lax.broadcasted_iota(jnp.int32, shape, 1)

    def table_rows(block_ref, table_ref, width):
        chosen = jnp.zeros(shape, jnp.int32)
        for k in range(n_blocks):
            chosen = jnp.where(row == k, block_ref[k], chosen)
        per_group = LANES // width
        found = jnp.zeros(shape, jnp.float32)
        for group in range(table_ref.shape[1] // LANES):
            part = table_ref[:, group * LANES : (group + 1) * LANES]
            found += jnp.where(lane // width + group * per_group == chosen, part, 0.0)
        shift = width
        while shift < LANES:
            found += pltpu.roll(found, shift, 1)
            shift *= 2
        return found

    occ = table_rows(occ_block, occ_ref, OB)
    vir = table_rows(vir_block, vir_ref, VB)
    mine = lax.axis_index("tm")
    n_times = len(taus)
    for part in range(OB * VB // LANES):
        level = jnp.take_along_axis(occ, lane // VB + part * (LANES // VB), axis=1)
        gap = level + vir
        total = jnp.zeros(shape, jnp.float32)
        for i in range(n_times):
            factor = jnp.float32(0.0)
            for j in range(n_times):
                factor = jnp.where(mine == j, jnp.float32(coef[j][i]), factor)
            total += factor * jnp.exp(-gap * taus[i])
        w_ref[:, part * LANES : (part + 1) * LANES] = total


def scale_rows(scaled, new, source, w_ref):
    width = w_ref.shape[1]
    for k in range(w_ref.shape[0]):
        cols = pl.ds(k * width, width)
        scaled[new, cols] = (source(cols).astype(jnp.float32) * w_ref[k : k + 1, :]).astype(jnp.bfloat16)


def multiply(scaled, right, here, out, arrived=None):
    total = lax.dot_general(scaled[...], right, (((1,), (1,)), ((), ())), preferred_element_type=jnp.float32)
    if arrived is not None:
        total += arrived[:, here].astype(jnp.float32)
    out[:, here] = total.astype(out.dtype)


def blocks_of(layers, n_pair, naux, z):
    if layers == 1:
        return [(0, 0, naux)]
    height = naux // (layers * n_pair)
    return [
        ((p * layers + jnp.bitwise_xor(z, layer)) * height, (layer * n_pair + p) * height, height)
        for layer in range(layers)
        for p in range(n_pair)
    ]


def first_kernel(taus, coef, layers, masks, rows, first, occ_block, vir_block, occ, vir, source, *refs):
    count = len(masks)
    w_ref, held, out = refs[:3]
    occ_b, vir_b, occ_t, vir_t, left, scaled, sems = refs[3:]
    naux = held.shape[0]
    me, z, n_pair = lax.axis_index("pair"), lax.axis_index("tm"), lax.axis_size("pair")
    small = ((occ_block, occ_b), (vir_block, vir_b), (occ, occ_t), (vir, vir_t))
    pairs = list(small)
    for b, mask in enumerate(masks):
        start = pl.multiple_of(jnp.bitwise_xor(me, mask) * rows, SUBLANES)
        pairs.append((source.at[pl.ds(start, rows), :], left.at[pl.ds(b * rows, rows), :]))
    blocks = blocks_of(layers, n_pair, naux, z)
    for old, new, length in blocks:
        pairs.append((source.at[pl.ds(pl.multiple_of(old, SUBLANES), length), :], held.at[pl.ds(new, length), :]))
    copies = [pltpu.make_async_copy(here, there, sems.at[i]) for i, (here, there) in enumerate(pairs)]
    for copy in copies:
        copy.start()
    for copy in copies[: len(small)]:
        copy.wait()
    weights_kernel(taus, coef, occ_b, vir_b, occ_t, vir_t, w_ref)
    for b in range(count):
        copies[len(small) + b].wait()
        here = pl.ds(b * rows, rows)
        scale_rows(scaled, here, lambda cols: left[here, cols], w_ref)
    waiting = list(zip(copies[len(small) + count :], blocks))
    width = out.shape[1]
    tile = math.gcd(width, TILE)
    for n in range(width // tile):
        while waiting and waiting[0][1][1] < first + (n + 1) * tile:
            waiting.pop(0)[0].wait()
        multiply(scaled, held[pl.ds(first + n * tile, tile), :], pl.ds(n * tile, tile), out)
    for copy, _ in waiting:
        copy.wait()


def first_rows(three_centre, occ_depth, vir_energy, occ_block, vir_block, masks, rows, layers, n_times, first, width):
    taus, coef = time_tables(n_times)
    _, depth = three_centre.shape
    count = len(masks)
    vmem = pl.BlockSpec(memory_space=pltpu.VMEM)
    operands = (occ_block, vir_block, occ_depth.reshape(1, -1), vir_energy.reshape(1, -1), three_centre)
    n_copies = 4 + count + (1 if layers == 1 else layers * lax.axis_size("pair"))
    return pl.pallas_call(
        functools.partial(first_kernel, taus, coef, layers, masks, rows, first),
        out_shape=[
            pltpu.VMEM((occ_block.shape[0], OB * VB), jnp.float32),
            pltpu.VMEM(three_centre.shape, three_centre.dtype),
            jax.ShapeDtypeStruct((count * rows, width), jnp.bfloat16),
        ],
        in_specs=[pl.BlockSpec(memory_space=pltpu.HBM)] * len(operands),
        out_specs=[vmem] * 3,
        scratch_shapes=[pltpu.SMEM(occ_block.shape, jnp.int32), pltpu.SMEM(vir_block.shape, jnp.int32)]
        + [pltpu.VMEM(v.shape, jnp.float32) for v in operands[2:4]]
        + [pltpu.VMEM((count * rows, depth), jnp.bfloat16)] * 2
        + [pltpu.SemaphoreType.DMA((n_copies,))],
        name="first",
        compiler_params=pltpu.CompilerParams(vmem_limit_bytes=24 * 2**20),
        cost_estimate=pl.CostEstimate(
            flops=2 * count * rows * width * depth, bytes_accessed=2 * three_centre.size, transcendentals=10**4
        ),
    )(*[pltpu.with_memory_space_constraint(v, pltpu.HBM) for v in operands])


def partial_kernel(masks, layers, first, has_arrived, w_ref, held, *refs):
    arrived = refs[0] if has_arrived else None
    out, scaled = refs[-2:]
    count = len(masks)
    rows, width = out.shape[0] // count, out.shape[1]
    me, z, n_pair = lax.axis_index("pair"), lax.axis_index("tm"), lax.axis_size("pair")
    height = rows // layers
    for b, mask in enumerate(masks):
        owner = jnp.bitwise_xor(me, mask)
        for part in range(layers):
            row = owner if layers == 1 else jnp.bitwise_xor(z, part) * n_pair + owner
            old = pl.ds(pl.multiple_of(row * height, SUBLANES), height)
            scale_rows(scaled, pl.ds(b * rows + part * height, height), lambda cols: held[old, cols], w_ref)
    tile = math.gcd(width, TILE)
    for n in range(width // tile):
        multiply(scaled, held[pl.ds(first + n * tile, tile), :], pl.ds(n * tile, tile), out, arrived)


def partial_rows(held, weights, masks, dtype, rows, layers, first, width, arrived=None):
    _, depth = held.shape
    count = len(masks)
    vmem = pl.BlockSpec(memory_space=pltpu.VMEM)
    operands = [pltpu.with_memory_space_constraint(v, pltpu.VMEM) for v in (weights, held)]
    operands += [] if arrived is None else [arrived]
    return pl.pallas_call(
        functools.partial(partial_kernel, masks, layers, first, arrived is not None),
        in_specs=[vmem] * len(operands),
        out_specs=vmem,
        scratch_shapes=[pltpu.VMEM((count * rows, depth), jnp.bfloat16)],
        out_shape=jax.ShapeDtypeStruct((count * rows, width), dtype),
        name="partial",
        compiler_params=pltpu.CompilerParams(vmem_limit_bytes=16 * 2**20),
        cost_estimate=pl.CostEstimate(
            flops=2 * count * rows * width * depth,
            bytes_accessed=2 * (width + count * rows) * depth + 4 * count * rows * width,
            transcendentals=0,
        ),
    )(*operands)


def pass_kernel(mine, other, out):
    rows = out.shape[0]
    out[...] = (mine[:rows].astype(jnp.float32) + other[:rows].astype(jnp.float32)).astype(out.dtype)


def pass_on(mine, other, rows):
    vmem = pl.BlockSpec(memory_space=pltpu.VMEM)
    width = mine.shape[1]
    return pl.pallas_call(
        pass_kernel,
        in_specs=[vmem] * 2,
        out_specs=vmem,
        out_shape=jax.ShapeDtypeStruct((rows, width), jnp.bfloat16),
        name="pass_on",
        compiler_params=pltpu.CompilerParams(vmem_limit_bytes=4 * 2**20),
        cost_estimate=pl.CostEstimate(flops=10**8, bytes_accessed=8 * rows * width, transcendentals=0),
    )(mine, other)


def lay(root, first_layer, last_layer, plan, pieces, height):
    me, z, n_pair = lax.axis_index("pair"), lax.axis_index("tm"), lax.axis_size("pair")
    for piece, (column, needed, blocks) in zip(pieces, plan):
        cols = pl.ds(column, piece.shape[1])

        def move():
            for i, (mask, layer) in enumerate(blocks):
                if first_layer <= layer < last_layer:
                    target = (jnp.bitwise_xor(me, mask) + (layer - first_layer) * n_pair) * height
                    root[pl.ds(pl.multiple_of(target, SUBLANES), height), cols] = piece[i * height : (i + 1) * height, :]

        if needed is None:
            move()
        else:
            pl.when(needed(z))(move)


def choose(pieces, first_layer, last_layer):
    kept = [p for p in pieces if any(first_layer <= layer < last_layer for _, layer in p[2])]
    return [p[:3] for p in kept], [p[3] for p in kept]


def collect_kernel(plan, last_layer, height, *refs):
    lay(refs[-1], 0, last_layer, plan, refs[:-1], height)


def collect(pieces, last_layer, height, naux):
    plan, values = choose(pieces, 0, last_layer)
    rows = last_layer * lax.axis_size("pair") * height
    vmem = pl.BlockSpec(memory_space=pltpu.VMEM)
    return pl.pallas_call(
        functools.partial(collect_kernel, plan, last_layer, height),
        in_specs=[vmem] * len(values),
        out_specs=vmem,
        out_shape=pltpu.VMEM((rows, naux), values[0].dtype),
        name="collect",
        compiler_params=pltpu.CompilerParams(vmem_limit_bytes=8 * 2**20),
        cost_estimate=pl.CostEstimate(flops=10**9, bytes_accessed=4 * rows * naux, transcendentals=0),
    )(*values)


def screen_kernel(plan, n_terms, *refs):
    terms = refs[:n_terms]
    root, out, chi = refs[n_terms:]
    rows = out.shape[0]
    sums = {}
    for term, (column, first) in zip(terms, plan):
        value = term[first : first + rows].astype(jnp.float32)
        sums[column] = value if column not in sums else sums[column] + value
    for column, value in sums.items():
        cols = pl.ds(column, value.shape[1])
        high = value.astype(jnp.bfloat16)
        chi[:rows, cols] = high
        chi[rows:, cols] = (value - high.astype(jnp.float32)).astype(jnp.bfloat16)
    tile = math.gcd(out.shape[1], TILE)
    for n in range(out.shape[1] // tile):
        cols = pl.ds(n * tile, tile)
        both = jnp.dot(chi[:, : root.shape[0]], root[:, cols], preferred_element_type=jnp.float32)
        out[:, cols] = both[:rows] + both[rows:]


def screen(terms, root, rows, naux):
    vmem = pl.BlockSpec(memory_space=pltpu.VMEM)
    return pl.pallas_call(
        functools.partial(screen_kernel, [t[:2] for t in terms], len(terms)),
        in_specs=[vmem] * (len(terms) + 1),
        out_specs=[vmem] * 2,
        out_shape=[
            jax.ShapeDtypeStruct((rows, root.shape[1]), jnp.float32),
            jax.ShapeDtypeStruct((2 * rows, naux), jnp.bfloat16),
        ],
        name="screen",
        compiler_params=pltpu.CompilerParams(vmem_limit_bytes=12 * 2**20),
        cost_estimate=pl.CostEstimate(
            flops=4 * rows * root.size, bytes_accessed=2 * root.size + 6 * rows * naux, transcendentals=0
        ),
    )(*[t[2] for t in terms], root)


def finish_kernel(plan, layer, height, total, chi, *refs):
    pieces, (out, root, staged, sems) = refs[: len(plan)], refs[len(plan) :]
    lay(root, layer, layer + 1, plan, pieces, height)
    depth, rows = root.shape[0], total.shape[0]
    tile = math.gcd(out.shape[2], TILE)
    copies = []
    for n in range(out.shape[2] // tile):
        cols = pl.ds(n * tile, tile)
        both = jnp.dot(chi[:, chi.shape[1] - depth :], root[:, cols], preferred_element_type=jnp.float32)
        staged[:, cols] = total[:, cols] + (both[:rows] + both[rows:])
        copies.append(pltpu.make_async_copy(staged.at[:, cols], out.at[0, :, cols], sems.at[n]))
        copies[-1].start()
    for copy in copies:
        copy.wait()


def finish(total, chi, pieces, layer, height):
    rows, naux = total.shape
    plan, values = choose(pieces, layer, layer + 1)
    depth = lax.axis_size("pair") * height
    vmem = pl.BlockSpec(memory_space=pltpu.VMEM)
    return pl.pallas_call(
        functools.partial(finish_kernel, plan, layer, height),
        in_specs=[vmem] * (2 + len(values)),
        out_specs=pl.BlockSpec(memory_space=pltpu.HBM),
        out_shape=jax.ShapeDtypeStruct((1, rows, naux), jnp.float32),
        scratch_shapes=[
            pltpu.VMEM((depth, naux), jnp.bfloat16),
            pltpu.VMEM((rows, naux), jnp.float32),
            pltpu.SemaphoreType.DMA((naux // math.gcd(naux, TILE),)),
        ],
        name="finish",
        compiler_params=pltpu.CompilerParams(vmem_limit_bytes=8 * 2**20),
        cost_estimate=pl.CostEstimate(
            flops=2 * rows * depth * naux, bytes_accessed=2 * depth * naux + 8 * rows * naux, transcendentals=0
        ),
    )(total, chi, *values)


def swap(value, mask):
    n_pair = lax.axis_size("pair")
    return lax.ppermute(value, "pair", [(p, p ^ mask) for p in range(n_pair)])


def along(value, moves):
    return lax.ppermute(value, "tm", moves)


def is_inner(z):
    return jnp.logical_or(z == 1, z == 2)


def is_outer(z):
    return jnp.logical_or(z == 0, z == 3)


def gather_root(root_coulomb):
    n_pair, n_tm = lax.axis_size("pair"), lax.axis_size("tm")
    masks = [2 * m for m in range(n_pair // 2)]
    near = [root_coulomb] + [swap(root_coulomb, m) for m in masks[1:]]
    plane = jnp.concatenate([rows[:, SPLIT:] for rows in near], axis=0)
    middle, outward = [(1, 2), (2, 1)], [(1, 0), (2, 3)]
    first = along(plane, [(z, z ^ 1) for z in range(n_tm)])
    second = along(plane, middle)
    inner = along(first, middle)
    outer = along(second, outward)
    last = along(inner, outward)
    pieces = []

    def both(column, needed, blocks, value):
        pieces.append((column, needed, blocks, value))
        pieces.append((column, needed, [(m ^ 1, layer) for m, layer in blocks], swap(value, 1)))

    for value, layer, needed in (
        (plane, 0, None),
        (first, 1, None),
        (second, 3, is_inner),
        (inner, 2, is_inner),
        (outer, 2, is_outer),
        (last, 3, is_outer),
    ):
        both(SPLIT, needed, [(m, layer) for m in masks], value)
    if SPLIT:
        tall = root_coulomb[:, :SPLIT]
        layers = range(n_tm)
        far = [tall] + [along(tall, [(z, z ^ m) for z in layers]) for m in layers[1:]]
        tower = jnp.concatenate(far, axis=0)
        for mask in masks:
            value = swap(tower, mask) if mask else tower
            both(0, None, [(mask, layer) for layer in layers], value)
    return pieces


def shards(layers, three_centre, root_coulomb, occ_depth, vir_energy, occ_block, vir_block):
    n_pair, n_tm = lax.axis_size("pair"), lax.axis_size("tm")
    height = root_coulomb.shape[0]
    naux = three_centre.shape[0]
    rows = naux // n_pair
    tables = (occ_depth, vir_energy, occ_block, vir_block)
    if layers == 1:
        return plain(three_centre, root_coulomb, tables, rows)
    pieces = gather_root(root_coulomb)
    root = collect(pieces, layers - 1, height, naux)
    x, y = 2, 4
    half = naux // 2
    jobs = {"a": ((x | y, x), 0), "b": ((x | y, y), half), "c": ((x, 0), half), "d": ((y, 0), 0)}
    others = {}
    for name, (masks, first) in jobs.items():
        masks = tuple(m ^ 1 for m in masks)
        if name == "a":
            weights, held, part = first_rows(three_centre, *tables, masks, rows, layers, n_tm, first, half)
        else:
            part = partial_rows(held, weights, masks, jnp.bfloat16, rows, layers, first, half)
        others[name] = swap(part, 1)
    sums = {}
    for name, (masks, first) in jobs.items():
        dtype = jnp.bfloat16 if name in "ab" else jnp.float32
        sums[name] = partial_rows(held, weights, masks, dtype, rows, layers, first, half, others[name])
    one_x = swap(sums["a"], x)
    one_y = swap(sums["b"], y)
    send_y = pass_on(sums["d"], one_x, rows)
    send_x = pass_on(sums["c"], one_y, rows)
    two_y = swap(send_y, y)
    two_x = swap(send_x, x)
    terms = [
        (0, rows, sums["d"]), (0, rows, one_x), (0, 0, two_y),
        (half, rows, sums["c"]), (half, rows, one_y), (half, 0, two_x),
    ]
    total, chi = screen(terms, root, rows, naux)
    return finish(total, chi, pieces, layers - 1, height)


def plain(three_centre, root_coulomb, tables, rows):
    n_pair, n_tm = lax.axis_size("pair"), lax.axis_size("tm")
    naux = three_centre.shape[0]
    root = lax.all_gather(root_coulomb, AXES, axis=0, tiled=True)
    terms = []
    groups = chip_groups(n_pair, rows)
    held = None
    for group in groups:
        masks = tuple(2 * m + 1 for m in group)
        if held is None:
            weights, held, part = first_rows(three_centre, *tables, masks, rows, 1, n_tm, 0, naux)
        else:
            part = partial_rows(held, weights, masks, jnp.bfloat16, rows, 1, 0, naux)
        other = swap(part, 1)
        own = partial_rows(held, weights, tuple(2 * m for m in group), jnp.float32, rows, 1, 0, naux, other)
        for i, m in enumerate(group):
            value = own[i * rows : (i + 1) * rows]
            terms.append((0, 0, swap(value.astype(jnp.bfloat16), 2 * m) if m else value))
    return screen(terms, root, rows, naux)[0][None]


def chip_groups(n_pair, rows):
    chips = sorted(range(n_pair // 2), key=lambda m: -popcount(m))
    size = max(1, min(len(chips), 384 // rows))
    return [chips[i : i + size] for i in range(0, len(chips), size)]


def solution(mesh):
    n_pair, n_tm = mesh.shape["pair"], mesh.shape["tm"]
    in_specs = (P(None, "pair"), P(("pair", "tm"), None), P(), P(), P("pair"), P("pair"))
    out_specs = P("tm", "pair", None)

    def step(*args):
        height = args[1].shape[0] // (n_pair * n_tm)
        line = n_tm == 4 and n_pair == 8 and height % SUBLANES == 0
        body = functools.partial(shards, n_tm if line else 1)
        return jax.shard_map(body, mesh=mesh, in_specs=in_specs, out_specs=out_specs, check_vma=False)(*args)

    return step
```

```python
import functools
import math

import numpy as np

import jax
import jax.numpy as jnp
from jax import lax
from jax.experimental import pallas as pl
from jax.experimental.pallas import tpu as pltpu
from jax.sharding import PartitionSpec as P


OB = 16
VB = 16
LANES = 128
SUBLANES = 16
TILE = 512
SPLIT = 768


AXES = ("pair", "tm")
LOG_SPAN = math.log(5000.0)


def popcount(mask):
    return bin(mask).count("1")


def time_tables(n_times):
    steps = np.arange(n_times).astype(np.float32)
    taus = (0.002 * np.exp(steps * np.float32(LOG_SPAN / max(n_times - 1, 1)))).astype(np.float32)
    omegas = ((steps + 0.5) / n_times).astype(np.float32)
    angle = np.float32(np.pi) * omegas[:, None] * (steps[None, :] + np.float32(0.5))
    coef = (np.float32(2.4) * omegas[:, None] * np.cos(angle)).astype(np.float32)
    return [float(t) for t in taus], [[float(c) for c in row] for row in coef]


def weights_kernel(taus, coef, occ_block, vir_block, occ_ref, vir_ref, w_ref):
    n_blocks = w_ref.shape[0]
    shape = (n_blocks, LANES)
    row = lax.broadcasted_iota(jnp.int32, shape, 0)
    lane = lax.broadcasted_iota(jnp.int32, shape, 1)

    def table_rows(block_ref, table_ref, width):
        chosen = jnp.zeros(shape, jnp.int32)
        for k in range(n_blocks):
            chosen = jnp.where(row == k, block_ref[k], chosen)
        per_group = LANES // width
        found = jnp.zeros(shape, jnp.float32)
        for group in range(table_ref.shape[1] // LANES):
            part = table_ref[:, group * LANES : (group + 1) * LANES]
            found += jnp.where(lane // width + group * per_group == chosen, part, 0.0)
        shift = width
        while shift < LANES:
            found += pltpu.roll(found, shift, 1)
            shift *= 2
        return found

    occ = table_rows(occ_block, occ_ref, OB)
    vir = table_rows(vir_block, vir_ref, VB)
    mine = lax.axis_index("tm")
    n_times = len(taus)
    for part in range(OB * VB // LANES):
        level = jnp.take_along_axis(occ, lane // VB + part * (LANES // VB), axis=1)
        gap = level + vir
        total = jnp.zeros(shape, jnp.float32)
        for i in range(n_times):
            factor = jnp.float32(0.0)
            for j in range(n_times):
                factor = jnp.where(mine == j, jnp.float32(coef[j][i]), factor)
            total += factor * jnp.exp(-gap * taus[i])
        w_ref[:, part * LANES : (part + 1) * LANES] = total


def scale_rows(scaled, new, source, w_ref):
    width = w_ref.shape[1]
    for k in range(w_ref.shape[0]):
        cols = pl.ds(k * width, width)
        scaled[new, cols] = (source(cols).astype(jnp.float32) * w_ref[k : k + 1, :]).astype(jnp.bfloat16)


def multiply(scaled, right, here, out, arrived=None):
    total = lax.dot_general(scaled[...], right, (((1,), (1,)), ((), ())), preferred_element_type=jnp.float32)
    if arrived is not None:
        total += arrived[:, here].astype(jnp.float32)
    out[:, here] = total.astype(out.dtype)


def blocks_of(layers, n_pair, naux, z):
    if layers == 1:
        return [(0, 0, naux)]
    height = naux // (layers * n_pair)
    return [
        ((p * layers + jnp.bitwise_xor(z, layer)) * height, (layer * n_pair + p) * height, height)
        for layer in range(layers)
        for p in range(n_pair)
    ]


def first_kernel(taus, coef, layers, masks, rows, first, occ_block, vir_block, occ, vir, source, *refs):
    count = len(masks)
    w_ref, held, out = refs[:3]
    occ_b, vir_b, occ_t, vir_t, left, scaled, sems = refs[3:]
    naux = held.shape[0]
    me, z, n_pair = lax.axis_index("pair"), lax.axis_index("tm"), lax.axis_size("pair")
    small = ((occ_block, occ_b), (vir_block, vir_b), (occ, occ_t), (vir, vir_t))
    pairs = list(small)
    for b, mask in enumerate(masks):
        start = pl.multiple_of(jnp.bitwise_xor(me, mask) * rows, SUBLANES)
        pairs.append((source.at[pl.ds(start, rows), :], left.at[pl.ds(b * rows, rows), :]))
    blocks = blocks_of(layers, n_pair, naux, z)
    for old, new, length in blocks:
        pairs.append((source.at[pl.ds(pl.multiple_of(old, SUBLANES), length), :], held.at[pl.ds(new, length), :]))
    copies = [pltpu.make_async_copy(here, there, sems.at[i]) for i, (here, there) in enumerate(pairs)]
    for copy in copies:
        copy.start()
    for copy in copies[: len(small)]:
        copy.wait()
    weights_kernel(taus, coef, occ_b, vir_b, occ_t, vir_t, w_ref)
    for b in range(count):
        copies[len(small) + b].wait()
        here = pl.ds(b * rows, rows)
        scale_rows(scaled, here, lambda cols: left[here, cols], w_ref)
    waiting = list(zip(copies[len(small) + count :], blocks))
    width = out.shape[1]
    tile = math.gcd(width, TILE)
    for n in range(width // tile):
        while waiting and waiting[0][1][1] < first + (n + 1) * tile:
            waiting.pop(0)[0].wait()
        multiply(scaled, held[pl.ds(first + n * tile, tile), :], pl.ds(n * tile, tile), out)
    for copy, _ in waiting:
        copy.wait()


def first_rows(three_centre, occ_depth, vir_energy, occ_block, vir_block, masks, rows, layers, n_times, first, width):
    taus, coef = time_tables(n_times)
    _, depth = three_centre.shape
    count = len(masks)
    vmem = pl.BlockSpec(memory_space=pltpu.VMEM)
    operands = (occ_block, vir_block, occ_depth.reshape(1, -1), vir_energy.reshape(1, -1), three_centre)
    n_copies = 4 + count + (1 if layers == 1 else layers * lax.axis_size("pair"))
    return pl.pallas_call(
        functools.partial(first_kernel, taus, coef, layers, masks, rows, first),
        out_shape=[
            pltpu.VMEM((occ_block.shape[0], OB * VB), jnp.float32),
            pltpu.VMEM(three_centre.shape, three_centre.dtype),
            jax.ShapeDtypeStruct((count * rows, width), jnp.bfloat16),
        ],
        in_specs=[pl.BlockSpec(memory_space=pltpu.HBM)] * len(operands),
        out_specs=[vmem] * 3,
        scratch_shapes=[pltpu.SMEM(occ_block.shape, jnp.int32), pltpu.SMEM(vir_block.shape, jnp.int32)]
        + [pltpu.VMEM(v.shape, jnp.float32) for v in operands[2:4]]
        + [pltpu.VMEM((count * rows, depth), jnp.bfloat16)] * 2
        + [pltpu.SemaphoreType.DMA((n_copies,))],
        name="first",
        compiler_params=pltpu.CompilerParams(vmem_limit_bytes=24 * 2**20),
        cost_estimate=pl.CostEstimate(
            flops=2 * count * rows * width * depth, bytes_accessed=2 * three_centre.size, transcendentals=10**4
        ),
    )(*[pltpu.with_memory_space_constraint(v, pltpu.HBM) for v in operands])


def partial_kernel(masks, layers, first, has_arrived, w_ref, held, *refs):
    arrived = refs[0] if has_arrived else None
    out, scaled = refs[-2:]
    count = len(masks)
    rows, width = out.shape[0] // count, out.shape[1]
    me, z, n_pair = lax.axis_index("pair"), lax.axis_index("tm"), lax.axis_size("pair")
    height = rows // layers
    for b, mask in enumerate(masks):
        owner = jnp.bitwise_xor(me, mask)
        for part in range(layers):
            row = owner if layers == 1 else jnp.bitwise_xor(z, part) * n_pair + owner
            old = pl.ds(pl.multiple_of(row * height, SUBLANES), height)
            scale_rows(scaled, pl.ds(b * rows + part * height, height), lambda cols: held[old, cols], w_ref)
    tile = math.gcd(width, TILE)
    for n in range(width // tile):
        multiply(scaled, held[pl.ds(first + n * tile, tile), :], pl.ds(n * tile, tile), out, arrived)


def partial_rows(held, weights, masks, dtype, rows, layers, first, width, arrived=None):
    _, depth = held.shape
    count = len(masks)
    vmem = pl.BlockSpec(memory_space=pltpu.VMEM)
    operands = [pltpu.with_memory_space_constraint(v, pltpu.VMEM) for v in (weights, held)]
    operands += [] if arrived is None else [arrived]
    return pl.pallas_call(
        functools.partial(partial_kernel, masks, layers, first, arrived is not None),
        in_specs=[vmem] * len(operands),
        out_specs=vmem,
        scratch_shapes=[pltpu.VMEM((count * rows, depth), jnp.bfloat16)],
        out_shape=jax.ShapeDtypeStruct((count * rows, width), dtype),
        name="partial",
        compiler_params=pltpu.CompilerParams(vmem_limit_bytes=16 * 2**20),
        cost_estimate=pl.CostEstimate(
            flops=2 * count * rows * width * depth,
            bytes_accessed=2 * (width + count * rows) * depth + 4 * count * rows * width,
            transcendentals=0,
        ),
    )(*operands)


def pass_kernel(mine, other, out):
    rows = out.shape[0]
    out[...] = (mine[:rows].astype(jnp.float32) + other[:rows].astype(jnp.float32)).astype(out.dtype)


def pass_on(mine, other, rows):
    vmem = pl.BlockSpec(memory_space=pltpu.VMEM)
    width = mine.shape[1]
    return pl.pallas_call(
        pass_kernel,
        in_specs=[vmem] * 2,
        out_specs=vmem,
        out_shape=jax.ShapeDtypeStruct((rows, width), jnp.bfloat16),
        name="pass_on",
        compiler_params=pltpu.CompilerParams(vmem_limit_bytes=4 * 2**20),
        cost_estimate=pl.CostEstimate(flops=10**8, bytes_accessed=8 * rows * width, transcendentals=0),
    )(mine, other)


def lay(root, first_layer, last_layer, plan, pieces, height):
    me, n_pair = lax.axis_index("pair"), lax.axis_size("pair")
    for piece, (column, blocks) in zip(pieces, plan):
        cols = pl.ds(column, piece.shape[1])
        for i, (mask, layer) in enumerate(blocks):
            if first_layer <= layer < last_layer:
                target = (jnp.bitwise_xor(me, mask) + (layer - first_layer) * n_pair) * height
                root[pl.ds(pl.multiple_of(target, SUBLANES), height), cols] = piece[i * height : (i + 1) * height, :]


def choose(pieces, first_layer, last_layer):
    kept = [p for p in pieces if any(first_layer <= layer < last_layer for _, layer in p[1])]
    return [p[:2] for p in kept], [p[2] for p in kept]


def collect_kernel(plan, last_layer, height, *refs):
    lay(refs[-1], 0, last_layer, plan, refs[:-1], height)


def collect(pieces, last_layer, height, naux):
    plan, values = choose(pieces, 0, last_layer)
    rows = last_layer * lax.axis_size("pair") * height
    vmem = pl.BlockSpec(memory_space=pltpu.VMEM)
    return pl.pallas_call(
        functools.partial(collect_kernel, plan, last_layer, height),
        in_specs=[vmem] * len(values),
        out_specs=vmem,
        out_shape=pltpu.VMEM((rows, naux), values[0].dtype),
        name="collect",
        compiler_params=pltpu.CompilerParams(vmem_limit_bytes=8 * 2**20),
        cost_estimate=pl.CostEstimate(flops=10**9, bytes_accessed=4 * rows * naux, transcendentals=0),
    )(*values)


def screen_kernel(plan, n_terms, *refs):
    terms = refs[:n_terms]
    root, out, chi = refs[n_terms:]
    rows = out.shape[0]
    sums = {}
    for term, (column, first) in zip(terms, plan):
        value = term[first : first + rows].astype(jnp.float32)
        sums[column] = value if column not in sums else sums[column] + value
    for column, value in sums.items():
        cols = pl.ds(column, value.shape[1])
        high = value.astype(jnp.bfloat16)
        chi[:rows, cols] = high
        chi[rows:, cols] = (value - high.astype(jnp.float32)).astype(jnp.bfloat16)
    tile = math.gcd(out.shape[1], TILE)
    for n in range(out.shape[1] // tile):
        cols = pl.ds(n * tile, tile)
        both = jnp.dot(chi[:, : root.shape[0]], root[:, cols], preferred_element_type=jnp.float32)
        out[:, cols] = both[:rows] + both[rows:]


def screen(terms, root, rows, naux):
    vmem = pl.BlockSpec(memory_space=pltpu.VMEM)
    return pl.pallas_call(
        functools.partial(screen_kernel, [t[:2] for t in terms], len(terms)),
        in_specs=[vmem] * (len(terms) + 1),
        out_specs=[vmem] * 2,
        out_shape=[
            jax.ShapeDtypeStruct((rows, root.shape[1]), jnp.float32),
            jax.ShapeDtypeStruct((2 * rows, naux), jnp.bfloat16),
        ],
        name="screen",
        compiler_params=pltpu.CompilerParams(vmem_limit_bytes=12 * 2**20),
        cost_estimate=pl.CostEstimate(
            flops=4 * rows * root.size, bytes_accessed=2 * root.size + 6 * rows * naux, transcendentals=0
        ),
    )(*[t[2] for t in terms], root)


def finish_kernel(plan, layer, height, total, chi, *refs):
    pieces, (out, root, staged, sems) = refs[: len(plan)], refs[len(plan) :]
    lay(root, layer, layer + 1, plan, pieces, height)
    depth, rows = root.shape[0], total.shape[0]
    tile = math.gcd(out.shape[2], TILE)
    copies = []
    for n in range(out.shape[2] // tile):
        cols = pl.ds(n * tile, tile)
        both = jnp.dot(chi[:, chi.shape[1] - depth :], root[:, cols], preferred_element_type=jnp.float32)
        staged[:, cols] = total[:, cols] + (both[:rows] + both[rows:])
        copies.append(pltpu.make_async_copy(staged.at[:, cols], out.at[0, :, cols], sems.at[n]))
        copies[-1].start()
    for copy in copies:
        copy.wait()


def finish(total, chi, pieces, layer, height):
    rows, naux = total.shape
    plan, values = choose(pieces, layer, layer + 1)
    depth = lax.axis_size("pair") * height
    vmem = pl.BlockSpec(memory_space=pltpu.VMEM)
    return pl.pallas_call(
        functools.partial(finish_kernel, plan, layer, height),
        in_specs=[vmem] * (2 + len(values)),
        out_specs=pl.BlockSpec(memory_space=pltpu.HBM),
        out_shape=jax.ShapeDtypeStruct((1, rows, naux), jnp.float32),
        scratch_shapes=[
            pltpu.VMEM((depth, naux), jnp.bfloat16),
            pltpu.VMEM((rows, naux), jnp.float32),
            pltpu.SemaphoreType.DMA((naux // math.gcd(naux, TILE),)),
        ],
        name="finish",
        compiler_params=pltpu.CompilerParams(vmem_limit_bytes=8 * 2**20),
        cost_estimate=pl.CostEstimate(
            flops=2 * rows * depth * naux, bytes_accessed=2 * depth * naux + 8 * rows * naux, transcendentals=0
        ),
    )(total, chi, *values)


def swap(value, mask):
    n_pair = lax.axis_size("pair")
    return lax.ppermute(value, "pair", [(p, p ^ mask) for p in range(n_pair)])


def along(value, layer):
    n_tm = lax.axis_size("tm")
    return lax.ppermute(value, "tm", [(z, z ^ layer) for z in range(n_tm)])


def gather_root(root_coulomb):
    n_pair, n_tm = lax.axis_size("pair"), lax.axis_size("tm")
    masks = [2 * m for m in range(n_pair // 2)]
    near = [root_coulomb] + [swap(root_coulomb, m) for m in masks[1:]]
    plane = jnp.concatenate([rows[:, SPLIT:] for rows in near], axis=0)
    layers = range(n_tm)
    pieces = []

    def both(column, blocks, value):
        pieces.append((column, blocks, value))
        pieces.append((column, [(m ^ 1, layer) for m, layer in blocks], swap(value, 1)))

    for layer in layers:
        value = along(plane, layer) if layer else plane
        both(SPLIT, [(m, layer) for m in masks], value)
    if SPLIT:
        tall = root_coulomb[:, :SPLIT]
        far = [tall] + [along(tall, layer) for layer in layers[1:]]
        tower = jnp.concatenate(far, axis=0)
        for mask in masks:
            value = swap(tower, mask) if mask else tower
            both(0, [(mask, layer) for layer in layers], value)
    return pieces


def shards(layers, three_centre, root_coulomb, occ_depth, vir_energy, occ_block, vir_block):
    n_pair, n_tm = lax.axis_size("pair"), lax.axis_size("tm")
    height = root_coulomb.shape[0]
    naux = three_centre.shape[0]
    rows = naux // n_pair
    tables = (occ_depth, vir_energy, occ_block, vir_block)
    if layers == 1:
        return plain(three_centre, root_coulomb, tables, rows)
    pieces = gather_root(root_coulomb)
    root = collect(pieces, layers - 1, height, naux)
    x, y = 2, 4
    half = naux // 2
    jobs = {"a": ((x | y, x), 0), "b": ((x | y, y), half), "c": ((x, 0), half), "d": ((y, 0), 0)}
    others = {}
    for name, (masks, first) in jobs.items():
        masks = tuple(m ^ 1 for m in masks)
        if name == "a":
            weights, held, part = first_rows(three_centre, *tables, masks, rows, layers, n_tm, first, half)
        else:
            part = partial_rows(held, weights, masks, jnp.bfloat16, rows, layers, first, half)
        others[name] = swap(part, 1)
    sums = {}
    for name, (masks, first) in jobs.items():
        dtype = jnp.bfloat16 if name in "ab" else jnp.float32
        sums[name] = partial_rows(held, weights, masks, dtype, rows, layers, first, half, others[name])
    one_x = swap(sums["a"], x)
    one_y = swap(sums["b"], y)
    send_y = pass_on(sums["d"], one_x, rows)
    send_x = pass_on(sums["c"], one_y, rows)
    two_y = swap(send_y, y)
    two_x = swap(send_x, x)
    terms = [
        (0, rows, sums["d"]), (0, rows, one_x), (0, 0, two_y),
        (half, rows, sums["c"]), (half, rows, one_y), (half, 0, two_x),
    ]
    total, chi = screen(terms, root, rows, naux)
    return finish(total, chi, pieces, layers - 1, height)


def plain(three_centre, root_coulomb, tables, rows):
    n_pair, n_tm = lax.axis_size("pair"), lax.axis_size("tm")
    naux = three_centre.shape[0]
    root = lax.all_gather(root_coulomb, AXES, axis=0, tiled=True)
    terms = []
    groups = chip_groups(n_pair, rows)
    held = None
    for group in groups:
        masks = tuple(2 * m + 1 for m in group)
        if held is None:
            weights, held, part = first_rows(three_centre, *tables, masks, rows, 1, n_tm, 0, naux)
        else:
            part = partial_rows(held, weights, masks, jnp.bfloat16, rows, 1, 0, naux)
        other = swap(part, 1)
        own = partial_rows(held, weights, tuple(2 * m for m in group), jnp.float32, rows, 1, 0, naux, other)
        for i, m in enumerate(group):
            value = own[i * rows : (i + 1) * rows]
            terms.append((0, 0, swap(value.astype(jnp.bfloat16), 2 * m) if m else value))
    return screen(terms, root, rows, naux)[0][None]


def chip_groups(n_pair, rows):
    chips = sorted(range(n_pair // 2), key=lambda m: -popcount(m))
    size = max(1, min(len(chips), 384 // rows))
    return [chips[i : i + size] for i in range(0, len(chips), size)]


def solution(mesh):
    n_pair, n_tm = mesh.shape["pair"], mesh.shape["tm"]
    in_specs = (P(None, "pair"), P(("pair", "tm"), None), P(), P(), P("pair"), P("pair"))
    out_specs = P("tm", "pair", None)

    def step(*args):
        height = args[1].shape[0] // (n_pair * n_tm)
        line = n_tm == 4 and n_pair == 8 and height % SUBLANES == 0
        body = functools.partial(shards, n_tm if line else 1)
        return jax.shard_map(body, mesh=mesh, in_specs=in_specs, out_specs=out_specs, check_vma=False)(*args)

    return step
```
